256 devices in a mesh: grp: 2 (over z), win: 128 (over y, x, core).
Axes of the slice: x: 8, y: 8, z: 2, core: 2. Of those that a mesh axis runs over, the one named last changes fastest.
The devices are a block of a 8x8x16 slice.
Arguments:
- tokens: bfloat16 [4, 8, 64, 384, 384], P('grp', None, None, 'win'), parts along dimension 0, may hold values from -6 to 6
- w_upper: bfloat16 [384, 640], replicated, may hold values from -0.3125 to 0.3125
- w_surface: bfloat16 [384, 256], replicated, may hold values from -0.3125 to 0.3125
- bias: float32 [69], replicated, may hold values from -1 to 1
Outputs:
- fields: bfloat16 [4, 17664, 1536], P('grp', 'win'), parts along dimension 0
The draws below stay inside these ranges and needn't reach their ends.
There are 2 independent parts, one for each index of `grp`. The reference program is written for one: setup_inputs(seed, part) draws one part's arguments, and reference() takes and returns one part's arrays. A program takes and returns all parts, laid end to end along the dimension named above; an argument that names none is the same for every part. Nothing has to cross between parts.
All inputs are finite; a program needn't handle non-finite values.
Results may differ from the reference program's by a relative error of at most 0.0048.
Values may be sent and summed in bfloat16 or wider, within the bound.
A program may use at most 128 MiB of HBM per device.

```python
import jax
import jax.numpy as jnp
from jax import lax

D = 384
VARS_UP = 5
LEVELS = 13
VARS_SF = 4
PATCH = 4
MEMB = 2
LAT_TOK = 64
LON_DEV = 3
LEV_TOK = 8
NLON = 384
OUT_CH = 69
N_WIN = 128


def steps_of(key, dims, split, least, largest):
    level, own = 1.0, jax.random.fold_in(key, 6)
    for dim, parts in split:
        steps = jnp.exp(jax.random.uniform(jax.random.fold_in(own, dim), (parts,), jnp.float32, least / len(split), largest / len(split)))
        level = level * jnp.repeat(steps, dims[dim] // parts).reshape([-1 if axis == dim else 1 for axis in range(len(dims))])
    return level


def normal_values(own_key, extent, scale, most, cuts=(), held_as=jnp.bfloat16):
    entries = scale * jax.random.normal(own_key, extent, jnp.float32)
    if cuts:
        entries = entries * steps_of(own_key, extent, cuts, -0.22, 0.18)
    return jnp.clip(entries, -most, most).astype(held_as)


def setup_inputs(seed: int = 0, part: int = 0) -> dict:
    streams_of = jax.random.split(jax.random.key(seed), 5)
    own_keys = jax.random.split(jax.random.fold_in(streams_of[4], part), 5)
    return {
        "tokens": normal_values(own_keys[0], (MEMB, LEV_TOK, LAT_TOK, NLON, D), 1.0, 6.0, ((3, 128),)),
        "w_upper": normal_values(streams_of[1], (D, VARS_UP * 8 * PATCH * PATCH), D ** -0.5, 0.3125),
        "w_surface": normal_values(streams_of[2], (D, VARS_SF * 4 * PATCH * PATCH), D ** -0.5, 0.3125),
        "bias": jnp.clip(jax.random.uniform(streams_of[3], (OUT_CH,), jnp.float32, -1.0, 1.0), -1.0, 1.0),
    }


def intersection_add(values, axis):
    first = lax.index_in_dim(values, 0, axis + 1, keepdims=False)
    second = lax.index_in_dim(values, 1, axis + 1, keepdims=False)
    pad_first = [(0, 0)] * first.ndim
    pad_second = [(0, 0)] * first.ndim
    pad_first[axis] = (0, 1)
    pad_second[axis] = (1, 0)
    return jnp.pad(first, pad_first) + jnp.pad(second, pad_second)


def project(tokens, w_upper, w_surface):
    members, tok_levels, lat_rows, lon_cols, width = tokens.shape
    upper_levels = tok_levels - 1
    rim_width = PATCH // 2
    upper = jnp.einsum("mzijd,dn->mzijn", tokens[:, :upper_levels], w_upper, preferred_element_type=jnp.float32)
    upper = upper.reshape(members, upper_levels, lat_rows, lon_cols, VARS_UP, 2, 2, PATCH, 2, PATCH)
    upper = jnp.transpose(upper, (0, 4, 1, 5, 2, 6, 7, 3, 8, 9))
    upper = intersection_add(upper, 4)
    upper = intersection_add(upper, 6)
    upper = upper.reshape(members, VARS_UP, 2 * upper_levels, (lat_rows + 1) * PATCH, (lon_cols + 1) * PATCH)
    upper = upper[:, :, :LEVELS, rim_width:rim_width + lat_rows * PATCH]
    upper = upper.reshape(members, VARS_UP * LEVELS, lat_rows * PATCH, (lon_cols + 1) * PATCH)
    surface = jnp.einsum("mijd,dn->mijn", tokens[:, upper_levels], w_surface, preferred_element_type=jnp.float32)
    surface = surface.reshape(members, lat_rows, lon_cols, VARS_SF, 2, PATCH, 2, PATCH)
    surface = jnp.transpose(surface, (0, 3, 1, 4, 5, 2, 6, 7))
    surface = intersection_add(surface, 2)
    surface = intersection_add(surface, 4)
    surface = surface.reshape(members, VARS_SF, (lat_rows + 1) * PATCH, (lon_cols + 1) * PATCH)
    surface = surface[:, :, rim_width:rim_width + lat_rows * PATCH]
    joined = jnp.concatenate([upper, surface], axis=1).astype(jnp.bfloat16)
    return joined.reshape(members, -1, (lon_cols + 1) * PATCH)


def reference(tokens, w_upper, w_surface, bias):
    members = tokens.shape[0]
    lat_rows = tokens.shape[2]
    rim_width = PATCH // 2

    def one_window(window):
        start = (window * LON_DEV).astype(jnp.int32)
        piece = lax.dynamic_slice_in_dim(tokens, start, LON_DEV, 3)
        return project(piece, w_upper, w_surface)

    frames = lax.map(one_window, jnp.arange(N_WIN, dtype=jnp.int32))
    frame_width = frames.shape[3]
    inner = frames[:, :, :, rim_width:frame_width - rim_width].astype(jnp.float32)
    columns = inner.shape[3]
    from_left = jnp.roll(frames[:, :, :, frame_width - rim_width:], 1, axis=0).astype(jnp.float32)
    from_right = jnp.roll(frames[:, :, :, :rim_width], -1, axis=0).astype(jnp.float32)
    edges = ((0, 0), (0, 0), (0, 0))
    summed = inner + jnp.pad(from_left, edges + ((0, columns - rim_width),))
    summed = summed + jnp.pad(from_right, edges + ((columns - rim_width, 0),))
    bias_rows = jnp.repeat(bias, lat_rows * PATCH)
    image = (summed + bias_rows[None, None, :, None]).astype(jnp.bfloat16)
    image = jnp.transpose(image, (1, 2, 0, 3))
    return image.reshape(members, image.shape[1], N_WIN * columns)
```

```python
import functools

import jax
import jax.numpy as jnp
from jax import lax
from jax.experimental import pallas as pl
from jax.experimental.pallas import tpu as pltpu
from jax.sharding import PartitionSpec as P

MESH = pl.DeviceIdType.MESH
BF = jnp.bfloat16
F32 = jnp.float32
VARS_UP = 5
LEVELS = 13
VARS_SF = 4
CHANNELS = VARS_UP * LEVELS + VARS_SF
LAT = 256
ROWS = CHANNELS * LAT // 128
TILES = ROWS + 2
NT = (((1,), (1,)), ((), ()))
SIDE = 8


def step_of(dy, dx):
    return ((dy - dx + SIDE) % SIDE) * SIDE + dx


def offset_of(s):
    dx = s % SIDE
    return (s // SIDE + dx) % SIDE, dx


def kernel_weights(w, kinds):
    width = w.shape[0]
    wt = jnp.transpose(w.reshape(width, kinds, 8, 8), (2, 1, 3, 0))

    def rows(lo, hi, before, after):
        return jnp.pad(wt[:, :, lo:hi], ((0, 0), (0, 0), (before, after), (0, 0)))

    def join(*parts):
        return jnp.concatenate(parts, -1).reshape(-1, width * len(parts))

    last = join(rows(6, 8, 0, 6), rows(2, 8, 0, 2), rows(0, 6, 2, 0))
    first = join(rows(2, 6, 0, 0), rows(0, 2, 2, 0))
    rims = join(rows(0, 2, 2, 0), rows(6, 8, 0, 2))
    return last, first, rims


def latitude(product_ref, kinds_rows, lane0):
    lane = lax.broadcasted_iota(jnp.int32, (1, 128), 1) % 64
    parts = []
    for b in range(4):
        main = product_ref[(b + 2) * kinds_rows : (b + 3) * kinds_rows, lane0 : lane0 + 128]
        a = (b + 6) % 8
        other = product_ref[a * kinds_rows : (a + 1) * kinds_rows, lane0 : lane0 + 128]
        if b < 2:
            moved = jnp.where(lane != 0, pltpu.roll(other, 1, 1), 0.0)
        else:
            moved = jnp.where(lane != 63, pltpu.roll(other, 127, 1), 0.0)
        parts.append((main + moved).astype(BF))
    return jnp.concatenate(parts, axis=1)


def kernel(
    n_chips,
    t_ref,
    ua_ref,
    ub_ref,
    ur_ref,
    sa_ref,
    sb_ref,
    sr_ref,
    bias_ref,
    perm_ref,
    got_ref,
    twin_ref,
    prod,
    image,
    rim_out,
    rim_in,
    chunks,
    rim_send,
    rim_recv,
    send_sem,
    recv_sem,
    own_sem,
    twin_send,
    twin_recv,
):
    n_win = 2 * n_chips
    w = lax.axis_index("win")
    chip, core = w // 2, w % 2
    y, x = chip // SIDE, chip % SIDE
    twin = chip * 2 + 1 - core
    right, left = (w + 1) % n_win, (w + n_win - 1) % n_win
    across = jnp.where(core == 1, right, left)

    barrier = pltpu.get_barrier_semaphore()

    def greet(s, _):
        other = ((chip + s) % n_chips) * 2 + core
        pl.semaphore_signal(barrier, 1, device_id={"win": other}, device_id_type=MESH)
        return 0

    lax.fori_loop(1, n_chips, greet, 0)
    pl.semaphore_signal(barrier, 1, device_id={"win": twin}, device_id_type=MESH)
    pl.semaphore_signal(barrier, 1, device_id={"win": across}, device_id_type=MESH)

    row8 = lax.broadcasted_iota(jnp.int32, (8, 128), 0)

    def columns(zs, j):
        return jnp.concatenate([t_ref[m, z, j] for z in zs for m in range(2)], axis=0)

    def halves(value, v):
        for h in range(2):
            first = value[8 * v : 8 * v + 8, h * 128 : h * 128 + 128]
            second = value[8 * v : 8 * v + 8, 256 + h * 128 : 256 + h * 128 + 128]
            yield h, jnp.where(row8 < 4, first, pltpu.roll(second, 4, 0)), jnp.where(
                row8 < 4, pltpu.roll(first, 4, 0), second
            )

    def rims(zs, w_ref, kinds, channel):
        rhs = jnp.concatenate([columns(zs, 0), columns(zs, 2)], axis=1)
        n = rhs.shape[0]
        rows = kinds * 4
        prod[: 8 * rows, :n] = lax.dot_general(w_ref[...], rhs, NT, preferred_element_type=F32)
        for zi in range(len(zs)):
            value = jnp.dot(
                latitude(prod, rows, zi * 128), perm_ref[...], preferred_element_type=F32
            )
            for v in range(kinds // 2):
                c0, c1 = channel(zi, 2 * v), channel(zi, 2 * v + 1)
                for h, one, two in halves(value, v):
                    rim_out[2 * c0 + h] = one.astype(BF)
                    rim_out[2 * c1 + h] = two.astype(BF)

    def inner(zs, a_ref, b_ref, kinds, channel):
        t01 = [columns(zs, 0), columns(zs, 1)]
        rhs = jnp.concatenate(t01 + [columns(zs, 2)], axis=1)
        n = rhs.shape[0]
        rows = kinds * 8
        prod[: 8 * rows, :n] = lax.dot_general(a_ref[...], rhs, NT, preferred_element_type=F32)
        for zi in range(len(zs)):
            value = jnp.dot(
                latitude(prod, rows, zi * 128), perm_ref[...], preferred_element_type=F32
            )
            for k in range(kinds):
                c = channel(zi, k)
                for m in range(2):
                    for h in range(2):
                        lo = m * 256 + h * 128
                        image[2 * c + h, m] = value[8 * k : 8 * k + 8, lo : lo + 128] + bias_ref[c]
        rhs = jnp.concatenate(t01, axis=1)
        rows = kinds * 4
        prod[: 8 * rows, :n] = lax.dot_general(b_ref[...], rhs, NT, preferred_element_type=F32)
        for zi in range(len(zs)):
            value = jnp.dot(
                latitude(prod, rows, zi * 128), perm_ref[...], preferred_element_type=F32
            )
            for v in range(kinds // 2):
                c0, c1 = channel(zi, 2 * v), channel(zi, 2 * v + 1)
                for h, one, two in halves(value, v):
                    image[2 * c0 + h, 2] = one + bias_ref[c0]
                    image[2 * c1 + h, 2] = two + bias_ref[c1]

    levels = t_ref.shape[1]
    pairs = levels // 2

    def upper_rims(q, _):
        p = pairs - 1 - q
        rims((2 * p, 2 * p + 1), ur_ref, 10, lambda zi, k: 13 * (k // 2) + 2 * (2 * p + zi) + k % 2)
        return 0

    def upper_inner(q, _):
        p = pairs - 1 - q
        inner(
            (2 * p, 2 * p + 1),
            ua_ref,
            ub_ref,
            10,
            lambda zi, k: 13 * (k // 2) + 2 * (2 * p + zi) + k % 2,
        )
        return 0

    def surface_channel(zi, k):
        return VARS_UP * LEVELS + k

    lax.fori_loop(0, pairs, upper_rims, 0)
    rims((levels - 1,), sr_ref, 4, surface_channel)

    pl.semaphore_wait(barrier, n_chips + 1)
    rim_copies = []
    for side, other in ((0, right), (1, left)):
        copy = pltpu.make_async_remote_copy(
            src_ref=rim_out,
            dst_ref=rim_in.at[side],
            send_sem=rim_send.at[side],
            recv_sem=rim_recv.at[side],
            device_id={"win": other},
            device_id_type=MESH,
        )
        copy.start()
        rim_copies.append(copy)

    lax.fori_loop(0, pairs, upper_inner, 0)
    inner((levels - 1,), sa_ref, sb_ref, 4, surface_channel)

    for copy in rim_copies:
        copy.wait()

    def add_rims(q, _):
        for u in range(6):
            t = q * 6 + u
            before = rim_in[0, t].astype(F32)
            after = rim_in[1, t].astype(F32)
            image[t, 2] += jnp.where(row8 % 4 < 2, before, 0.0)
            image[t, 0] += jnp.where(row8 >= 6, pltpu.roll(after, 4, 0), 0.0)
            image[t, 1] += jnp.where(row8 >= 6, after, 0.0)
        return 0

    lax.fori_loop(0, ROWS // 6, add_rims, 0)

    lane = lax.broadcasted_iota(jnp.int32, (8, 128), 1)

    def send_copy(s):
        dy, dx = offset_of(s)
        to = ((y + dy) % SIDE) * SIDE + (x + dx) % SIDE
        return to, pltpu.make_async_remote_copy(
            src_ref=chunks.at[s],
            dst_ref=got_ref.at[s],
            send_sem=send_sem.at[s],
            recv_sem=recv_sem.at[s],
            device_id={"win": to * 2 + core},
            device_id_type=MESH,
        )

    def make_chunk(s, to):
        tails = jnp.zeros((8, 128), F32)
        for k in range(2):
            d = to * 2 + k
            t = (d * ROWS) // 128
            o = (d * ROWS) % 128
            back = (128 - o) % 128
            for g in range(3):
                a = pltpu.roll(image[t, g], back, 1)
                b = pltpu.roll(image[t + 1, g], back, 1)
                c = pltpu.roll(image[t + 2, g], back, 1)
                chunks[s, 4 * k + g] = jnp.where(lane < 128 - o, a, b).astype(BF)
                tail = jnp.where(lane < 128 - o, b, c)
                for slot in (g,) if g < 2 else (2, 3):
                    at = 64 * k + 16 * slot
                    moved = pltpu.roll(tail, at, 1) if at else tail
                    tails = jnp.where((lane >= at) & (lane < at + 10), moved, tails)
        chunks[s, 3] = tails.astype(BF)

    make_chunk(0, chip)
    own = pltpu.make_async_copy(chunks.at[0], got_ref.at[0], own_sem)
    own.start()

    def exchange(s, _):
        to, copy = send_copy(s)
        make_chunk(s, to)
        copy.start()
        return 0

    lax.fori_loop(1, n_chips, exchange, 0)
    own.wait()

    def twin_copy(g):
        part = pl.ds(g * SIDE, SIDE)
        return pltpu.make_async_remote_copy(
            src_ref=got_ref.at[part, pl.ds(3 * (1 - core), 4)],
            dst_ref=twin_ref.at[part],
            send_sem=twin_send.at[g],
            recv_sem=twin_recv.at[g],
            device_id={"win": twin},
            device_id_type=MESH,
        )

    def arrived(s, _):
        send_copy(s)[1].wait_recv()
        return 0

    for g in range(n_chips // SIDE):
        lax.fori_loop(max(1, g * SIDE), (g + 1) * SIDE, arrived, 0)
        twin_copy(g).start()

    def left_here(s, _):
        send_copy(s)[1].wait_send()
        return 0

    lax.fori_loop(1, n_chips, left_here, 0)
    for g in range(n_chips // SIDE):
        twin_copy(g).wait()


def finish(n_chips, got_ref, twin_ref, out_ref):
    w = lax.axis_index("win")
    chip, core = w // 2, w % 2
    y, x = chip // SIDE, chip % SIDE
    first = core == 0
    row = lax.broadcasted_iota(jnp.int32, (8, 128), 0)
    lane = lax.broadcasted_iota(jnp.int32, (8, 128), 1)
    top = row < 4
    spot = lane - 64 * core
    bands = ((spot >= 0) & (spot < 10)) | ((spot >= 16) & (spot < 26))
    third = (spot >= 32) & (spot < 42)
    fourth = (spot >= 48) & (spot < 58)

    def select(mask, value):
        return jnp.where(mask, value, 0.0)

    r = lax.broadcasted_iota(jnp.int32, (2 * ROWS, 384), 0)
    k = lax.broadcasted_iota(jnp.int32, (2 * ROWS, 384), 1)
    rho, m = r // 2, r % 2
    at = 256 + 64 * core + 16 * m + rho - 128
    hot = ((rho < 128) & (k == 128 * m + rho)) | ((rho >= 128) & ((k == at) | (k == at + 32)))
    pick = jnp.where(hot, 1.0, 0.0).astype(BF)

    for block in range(n_chips // 16):
        pieces = []
        for i in range(16):
            p = block * 16 + i
            s = step_of((y - p // SIDE + SIDE) % SIDE, (x - p % SIDE + SIDE) % SIDE)
            mine = [got_ref[s, 3 * core + u].astype(F32) for u in range(4)]
            other = [twin_ref[s, u].astype(F32) for u in range(4)]
            mine = [jnp.where(first, mine[u], mine[(u + 1) % 4]) for u in range(4)]
            other = [jnp.where(first, other[u], other[(u + 1) % 4]) for u in range(4)]
            a = [jnp.where(first, mine[u], other[u]) for u in range(4)]
            b = [jnp.where(first, other[u], mine[u]) for u in range(4)]
            blocks = []
            for mm in range(2):
                ra = pltpu.roll(a[mm], 4, 0)
                if mm == 0:
                    rows = [
                        jnp.where(top, a[2], ra),
                        jnp.where(top, ra, pltpu.roll(b[2], 4, 0)),
                        b[0],
                    ]
                else:
                    rows = [
                        jnp.where(top, pltpu.roll(a[2], 4, 0), ra),
                        jnp.where(top, ra, b[2]),
                        b[1],
                    ]
                blocks.append(jnp.concatenate(rows, axis=0))
            ta, tb = a[3], b[3]
            ra, rb = pltpu.roll(ta, 4, 0), pltpu.roll(tb, 4, 0)
            rows = [
                jnp.where(top, select(third, ta) + select(fourth, ra), select(bands, ra)),
                jnp.where(top, select(bands, ra), select(third, rb) + select(fourth, tb)),
                select(bands, tb),
            ]
            blocks.append(jnp.concatenate(rows, axis=0))
            pieces.append(jnp.concatenate(blocks, axis=1))
        stacked = jnp.concatenate(pieces, axis=0).astype(BF)
        out_ref[:, block * 384 : block * 384 + 384] = lax.dot_general(
            pick, stacked, NT, preferred_element_type=F32
        ).astype(BF)


def interleave():
    k = jnp.arange(512)
    b, m, i = k // 128, (k // 64) % 2, k % 64
    target = m * LAT + 4 * i + b
    return (target[:, None] == jnp.arange(512)[None, :]).astype(BF)


def body(n_chips, tokens, w_upper, w_surface, bias):
    t = jnp.transpose(tokens, (0, 1, 3, 2, 4))
    ua, ub, ur = kernel_weights(w_upper, 10)
    sa, sb, sr = kernel_weights(w_surface, 4)
    vmem = pl.BlockSpec(memory_space=pltpu.VMEM)
    smem = pl.BlockSpec(memory_space=pltpu.SMEM)
    anywhere = pl.BlockSpec(memory_space=pl.ANY)
    dma = pltpu.SemaphoreType.DMA
    got, twin = pl.pallas_call(
        functools.partial(kernel, n_chips),
        out_shape=(
            jax.ShapeDtypeStruct((n_chips, 7, 8, 128), BF),
            jax.ShapeDtypeStruct((n_chips, 4, 8, 128), BF),
        ),
        in_specs=[vmem] * 7 + [smem, vmem],
        out_specs=(anywhere, anywhere),
        scratch_shapes=[
            pltpu.VMEM((640, 256), F32),
            pltpu.VMEM((TILES, 3, 8, 128), F32),
            pltpu.VMEM((TILES, 8, 128), BF),
            pltpu.VMEM((2, TILES, 8, 128), BF),
            pltpu.VMEM((n_chips, 7, 8, 128), BF),
            dma((2,)),
            dma((2,)),
            dma((n_chips,)),
            dma((n_chips,)),
            dma,
            dma((n_chips // SIDE,)),
            dma((n_chips // SIDE,)),
        ],
        compiler_params=pltpu.CompilerParams(
            collective_id=0, has_side_effects=True, vmem_limit_bytes=40 * 2**20
        ),
        name="recover",
    )(t, ua, ub, ur, sa, sb, sr, bias, interleave())
    rows = pl.pallas_call(
        functools.partial(finish, n_chips),
        out_shape=jax.ShapeDtypeStruct((2 * ROWS, n_chips * 24), BF),
        in_specs=[vmem, vmem],
        out_specs=vmem,
        compiler_params=pltpu.CompilerParams(vmem_limit_bytes=40 * 2**20),
        name="finish",
    )(got, twin)
    return jnp.transpose(rows.reshape(ROWS, 2, n_chips * 24), (1, 0, 2))


def solution(mesh):
    n_chips = mesh.shape["win"] // 2
    return jax.shard_map(
        functools.partial(body, n_chips),
        mesh=mesh,
        in_specs=(P("grp", None, None, "win", None), P(), P(), P()),
        out_specs=P("grp", "win", None),
        check_vma=False,
    )
```

```python
import functools

import jax
import jax.numpy as jnp
from jax import lax
from jax.experimental import pallas as pl
from jax.experimental.pallas import tpu as pltpu
from jax.sharding import PartitionSpec as P

MESH = pl.DeviceIdType.MESH
BF = jnp.bfloat16
F32 = jnp.float32
VARS_UP = 5
LEVELS = 13
VARS_SF = 4
CHANNELS = VARS_UP * LEVELS + VARS_SF
LAT = 256
ROWS = CHANNELS * LAT // 128
TILES = ROWS + 2
NT = (((1,), (1,)), ((), ()))
SIDE = 8


def step_of(dy, dx):
    return ((dy - dx + SIDE) % SIDE) * SIDE + dx


def offset_of(s):
    dx = s % SIDE
    return (s // SIDE + dx) % SIDE, dx


def prepare(w_ref, kinds, last_ref, first_ref, rims_ref):
    width = w_ref.shape[0]
    row = lax.broadcasted_iota(jnp.int32, (8, width), 0)
    a = lax.broadcasted_iota(jnp.int32, (128, 128), 0)
    b = lax.broadcasted_iota(jnp.int32, (128, 128), 1)
    unit = jnp.where(a == b, 1.0, 0.0).astype(BF)

    def keep(mask, value):
        return jnp.where(mask, value, 0.0)

    turned = [
        lax.dot_general(unit, w_ref[:, i * 128 : i * 128 + 128], NT, preferred_element_type=F32)
        for i in range(kinds // 2)
    ]
    for pair in range(kinds // 2):
        for lat in range(8):
            down, up = [], []
            for k in range(2):
                eight = turned[pair][k * 64 + lat * 8 : k * 64 + lat * 8 + 8]
                down.append(pltpu.roll(eight, 2, 0))
                up.append(pltpu.roll(eight, 6, 0))
            at = (lat * kinds + 2 * pair) * 8
            parts = [
                [keep(row < 2, down[k]), keep(row < 6, up[k]), keep(row >= 2, down[k])]
                for k in range(2)
            ]
            for j in range(3):
                both = jnp.concatenate([parts[0][j], parts[1][j]], axis=0)
                last_ref[at : at + 16, j * width : (j + 1) * width] = both.astype(BF)
            half = at // 2
            outer = keep((row == 2) | (row == 3), down[0]) + keep(row >= 6, up[1])
            middle = jnp.where(row < 4, up[0], down[1])
            first_ref[half : half + 8, :width] = middle.astype(BF)
            first_ref[half : half + 8, width:] = outer.astype(BF)
            tail = keep(row < 2, down[0]) + keep((row == 4) | (row == 5), up[1])
            rims_ref[half : half + 8, :width] = outer.astype(BF)
            rims_ref[half : half + 8, width:] = tail.astype(BF)


def latitude(product_ref, rows, lane0):
    place = lax.broadcasted_iota(jnp.int32, (rows, 128), 1)
    lane = place % 64
    parts = []
    for b in range(4):
        main = product_ref[(b + 2) * rows : (b + 3) * rows, lane0 : lane0 + 128]
        a = (b + 6) % 8
        other = product_ref[a * rows : (a + 1) * rows, lane0 : lane0 + 128]
        if b < 2:
            moved = jnp.where(lane != 0, pltpu.roll(other, 1, 1), 0.0)
        else:
            moved = jnp.where(lane != 63, pltpu.roll(other, 127, 1), 0.0)
        parts.append(main + moved)
    low = place < 64
    turned = [pltpu.roll(p, 64, 1) for p in parts]
    return [
        jnp.concatenate(
            [jnp.where(low, parts[0], turned[1]), jnp.where(low, parts[2], turned[3])], axis=1
        ),
        jnp.concatenate(
            [jnp.where(low, turned[0], parts[1]), jnp.where(low, turned[2], parts[3])], axis=1
        ),
    ]


def kernel(
    n_chips,
    t_ref,
    wu_any,
    ws_any,
    bias_ref,
    out_ref,
    got_ref,
    twin_ref,
    held,
    wu_ref,
    ws_ref,
    ua_ref,
    ub_ref,
    ur_ref,
    sa_ref,
    sb_ref,
    sr_ref,
    perm_ref,
    prod_a,
    prod_b,
    token_sem,
    image,
    rim_out,
    rim_in,
    chunks,
    rim_send,
    rim_recv,
    send_sem,
    recv_sem,
    twin_send,
    twin_recv,
):
    n_win = 2 * n_chips
    w = lax.axis_index("win")
    chip, core = w // 2, w % 2
    y, x = chip // SIDE, chip % SIDE
    twin = chip * 2 + 1 - core
    right, left = (w + 1) % n_win, (w + n_win - 1) % n_win
    across = jnp.where(core == 1, right, left)

    levels = t_ref.shape[1]
    pairs = levels // 2

    def token_copy(z):
        return pltpu.make_async_copy(t_ref.at[:, z], held.at[:, z], token_sem.at[z])

    weight_copies = [
        pltpu.make_async_copy(wu_any, wu_ref, token_sem.at[levels]),
        pltpu.make_async_copy(ws_any, ws_ref, token_sem.at[levels + 1]),
    ]
    for copy in weight_copies:
        copy.start()
    for z in range(levels - 1, -1, -1):
        token_copy(z).start()

    barrier = pltpu.get_barrier_semaphore()

    def greet(s, _):
        other = ((chip + s) % n_chips) * 2 + core
        pl.semaphore_signal(barrier, 1, device_id={"win": other}, device_id_type=MESH)
        return 0

    lax.fori_loop(1, n_chips, greet, 0)
    pl.semaphore_signal(barrier, 1, device_id={"win": twin}, device_id_type=MESH)
    pl.semaphore_signal(barrier, 1, device_id={"win": across}, device_id_type=MESH)

    k256 = lax.broadcasted_iota(jnp.int32, (LAT, LAT), 0)
    n256 = lax.broadcasted_iota(jnp.int32, (LAT, LAT), 1)
    perm_ref[...] = jnp.where(4 * (k256 % 64) + k256 // 64 == n256, 1.0, 0.0).astype(BF)
    weight_copies[0].wait()
    prepare(wu_ref, 2 * VARS_UP, ua_ref, ub_ref, ur_ref)
    weight_copies[1].wait()
    prepare(ws_ref, VARS_SF, sa_ref, sb_ref, sr_ref)

    row8 = lax.broadcasted_iota(jnp.int32, (8, 128), 0)

    def columns(zs, j):
        return jnp.concatenate([held[m, z, j] for z in zs for m in range(2)], axis=0)

    def halves(values, at):
        for h in range(2):
            first = values[0][at : at + 8, h * 128 : h * 128 + 128]
            second = values[1][at : at + 8, h * 128 : h * 128 + 128]
            yield h, jnp.where(row8 < 4, first, pltpu.roll(second, 4, 0)), jnp.where(
                row8 < 4, pltpu.roll(first, 4, 0), second
            )

    def interleaved(blocks):
        stacked = jnp.concatenate([b.astype(BF) for b in blocks], axis=0)
        value = jnp.dot(stacked, perm_ref[...], preferred_element_type=F32)
        out, at = [], 0
        for b in blocks:
            out.append(value[at : at + b.shape[0]])
            at += b.shape[0]
        return out

    def per_member(product_ref, rows, count):
        found = [latitude(product_ref, rows, zi * 128) for zi in range(count)]
        return [jnp.concatenate([f[m] for f in found], axis=0) for m in range(2)]

    def rims(zs, w_ref, kinds, channel):
        rhs = jnp.concatenate([columns(zs, 0), columns(zs, 2)], axis=1)
        n = rhs.shape[0]
        rows = kinds * 4
        prod_b[: 8 * rows, :n] = lax.dot_general(w_ref[...], rhs, NT, preferred_element_type=F32)
        values = interleaved(per_member(prod_b, rows, len(zs)))
        for zi in range(len(zs)):
            for v in range(kinds // 2):
                c0, c1 = channel(zi, 2 * v), channel(zi, 2 * v + 1)
                for h, one, two in halves(values, zi * rows + 8 * v):
                    rim_out[2 * c0 + h] = one.astype(BF)
                    rim_out[2 * c1 + h] = two.astype(BF)

    def inner(zs, a_ref, b_ref, kinds, channel):
        t01 = [columns(zs, 0), columns(zs, 1)]
        rhs = jnp.concatenate(t01 + [columns(zs, 2)], axis=1)
        n = rhs.shape[0]
        rows_a, rows_b = kinds * 8, kinds * 4
        prod_a[: 8 * rows_a, :n] = lax.dot_general(a_ref[...], rhs, NT, preferred_element_type=F32)
        rhs = jnp.concatenate(t01, axis=1)
        prod_b[: 8 * rows_b, :n] = lax.dot_general(b_ref[...], rhs, NT, preferred_element_type=F32)
        values = interleaved(
            per_member(prod_a, rows_a, len(zs)) + per_member(prod_b, rows_b, len(zs))
        )
        for zi in range(len(zs)):
            for k in range(kinds):
                c = channel(zi, k)
                at = zi * rows_a + 8 * k
                for m in range(2):
                    for h in range(2):
                        lo = h * 128
                        image[2 * c + h, m] = values[m][at : at + 8, lo : lo + 128] + bias_ref[c]
            for v in range(kinds // 2):
                c0, c1 = channel(zi, 2 * v), channel(zi, 2 * v + 1)
                for h, one, two in halves(values[2:], zi * rows_b + 8 * v):
                    image[2 * c0 + h, 2] = one + bias_ref[c0]
                    image[2 * c1 + h, 2] = two + bias_ref[c1]

    def upper_rims(q, _):
        p = pairs - 1 - q
        token_copy(2 * p + 1).wait()
        token_copy(2 * p).wait()
        rims((2 * p, 2 * p + 1), ur_ref, 10, lambda zi, k: 13 * (k // 2) + 2 * (2 * p + zi) + k % 2)
        return 0

    def upper_inner(q, _):
        p = pairs - 1 - q
        inner(
            (2 * p, 2 * p + 1),
            ua_ref,
            ub_ref,
            10,
            lambda zi, k: 13 * (k // 2) + 2 * (2 * p + zi) + k % 2,
        )
        return 0

    def surface_channel(zi, k):
        return VARS_UP * LEVELS + k

    lax.fori_loop(0, pairs, upper_rims, 0)
    rims((levels - 1,), sr_ref, 4, surface_channel)

    def all_inner():
        lax.fori_loop(0, pairs, upper_inner, 0)
        inner((levels - 1,), sa_ref, sb_ref, 4, surface_channel)

    late = (y >= SIDE // 2) | (chip == 0)
    pl.when(jnp.logical_not(late))(all_inner)
    pl.semaphore_wait(barrier, n_chips + 1)
    rim_copies = []
    for side, other in ((0, right), (1, left)):
        copy = pltpu.make_async_remote_copy(
            src_ref=rim_out,
            dst_ref=rim_in.at[side],
            send_sem=rim_send.at[side],
            recv_sem=rim_recv.at[side],
            device_id={"win": other},
            device_id_type=MESH,
        )
        copy.start()
        rim_copies.append(copy)

    pl.when(late)(all_inner)

    for copy in rim_copies:
        copy.wait()

    def add_rims(q, _):
        for u in range(6):
            t = q * 6 + u
            before = rim_in[0, t].astype(F32)
            after = rim_in[1, t].astype(F32)
            image[t, 2] += jnp.where(row8 % 4 < 2, before, 0.0)
            image[t, 0] += jnp.where(row8 >= 6, pltpu.roll(after, 4, 0), 0.0)
            image[t, 1] += jnp.where(row8 >= 6, after, 0.0)
        return 0

    lax.fori_loop(0, ROWS // 6, add_rims, 0)

    lane = lax.broadcasted_iota(jnp.int32, (8, 128), 1)

    def send_copy(s):
        dy, dx = offset_of(s)
        to = ((y + dy) % SIDE) * SIDE + (x + dx) % SIDE
        return to, pltpu.make_async_remote_copy(
            src_ref=chunks.at[s],
            dst_ref=got_ref.at[s],
            send_sem=send_sem.at[s],
            recv_sem=recv_sem.at[s],
            device_id={"win": to * 2 + core},
            device_id_type=MESH,
        )

    def make_chunk(s, to):
        tails = jnp.zeros((8, 128), F32)
        for k in range(2):
            d = to * 2 + k
            t = (d * ROWS) // 128
            o = (d * ROWS) % 128
            back = (128 - o) % 128
            for g in range(3):
                a = pltpu.roll(image[t, g], back, 1)
                b = pltpu.roll(image[t + 1, g], back, 1)
                c = pltpu.roll(image[t + 2, g], back, 1)
                chunks[s, 4 * k + g] = jnp.where(lane < 128 - o, a, b).astype(BF)
                tail = jnp.where(lane < 128 - o, b, c)
                for slot in (g,) if g < 2 else (2, 3):
                    at = 64 * k + 16 * slot
                    moved = pltpu.roll(tail, at, 1) if at else tail
                    tails = jnp.where((lane >= at) & (lane < at + 10), moved, tails)
        chunks[s, 3] = tails.astype(BF)

    make_chunk(0, chip)
    got_ref[0] = chunks[0]

    def exchange(q, _):
        for u in range(3):
            s = 1 + q * 3 + u
            to, copy = send_copy(s)
            make_chunk(s, to)
            copy.start()
        return 0

    lax.fori_loop(0, (n_chips - 1) // 3, exchange, 0)
    def twin_copy(g):
        part = pl.ds(g * SIDE, SIDE)
        return pltpu.make_async_remote_copy(
            src_ref=got_ref.at[part, pl.ds(3 * (1 - core), 4)],
            dst_ref=twin_ref.at[part],
            send_sem=twin_send.at[g],
            recv_sem=twin_recv.at[g],
            device_id={"win": twin},
            device_id_type=MESH,
        )

    def arrived(s, _):
        send_copy(s)[1].wait_recv()
        return 0

    for g in range(n_chips // SIDE):
        lax.fori_loop(max(1, g * SIDE), (g + 1) * SIDE, arrived, 0)
        twin_copy(g).start()

    def left_here(s, _):
        send_copy(s)[1].wait_send()
        return 0

    lax.fori_loop(1, n_chips, left_here, 0)
    for g in range(n_chips // SIDE):
        twin_copy(g).wait()
    finish(n_chips, y, x, core, got_ref, twin_ref, out_ref)


def finish(n_chips, y, x, core, got_ref, twin_ref, out_ref):
    first = core == 0
    row = lax.broadcasted_iota(jnp.int32, (8, 128), 0)
    lane = lax.broadcasted_iota(jnp.int32, (8, 128), 1)
    top = row < 4
    spot = lane - 64 * core
    bands = ((spot >= 0) & (spot < 10)) | ((spot >= 16) & (spot < 26))
    third = (spot >= 32) & (spot < 42)
    fourth = (spot >= 48) & (spot < 58)

    def select(mask, value):
        return jnp.where(mask, value, 0.0)

    r = lax.broadcasted_iota(jnp.int32, (2 * ROWS, 384), 0)
    k = lax.broadcasted_iota(jnp.int32, (2 * ROWS, 384), 1)
    rho, m = r // 2, r % 2
    at = 256 + 64 * core + 16 * m + rho - 128
    hot = ((rho < 128) & (k == 128 * m + rho)) | ((rho >= 128) & ((k == at) | (k == at + 32)))
    pick = jnp.where(hot, 1.0, 0.0).astype(BF)

    for block in range(n_chips // 16):
        pieces = []
        for i in range(16):
            p = block * 16 + i
            s = step_of((y - p // SIDE + SIDE) % SIDE, (x - p % SIDE + SIDE) % SIDE)
            mine = [got_ref[s, 3 * core + u].astype(F32) for u in range(4)]
            other = [twin_ref[s, u].astype(F32) for u in range(4)]
            mine = [jnp.where(first, mine[u], mine[(u + 1) % 4]) for u in range(4)]
            other = [jnp.where(first, other[u], other[(u + 1) % 4]) for u in range(4)]
            a = [jnp.where(first, mine[u], other[u]) for u in range(4)]
            b = [jnp.where(first, other[u], mine[u]) for u in range(4)]
            blocks = []
            for mm in range(2):
                ra = pltpu.roll(a[mm], 4, 0)
                if mm == 0:
                    rows = [
                        jnp.where(top, a[2], ra),
                        jnp.where(top, ra, pltpu.roll(b[2], 4, 0)),
                        b[0],
                    ]
                else:
                    rows = [
                        jnp.where(top, pltpu.roll(a[2], 4, 0), ra),
                        jnp.where(top, ra, b[2]),
                        b[1],
                    ]
                blocks.append(jnp.concatenate(rows, axis=0))
            ta, tb = a[3], b[3]
            ra, rb = pltpu.roll(ta, 4, 0), pltpu.roll(tb, 4, 0)
            rows = [
                jnp.where(top, select(third, ta) + select(fourth, ra), select(bands, ra)),
                jnp.where(top, select(bands, ra), select(third, rb) + select(fourth, tb)),
                select(bands, tb),
            ]
            blocks.append(jnp.concatenate(rows, axis=0))
            pieces.append(jnp.concatenate(blocks, axis=1))
        stacked = jnp.concatenate(pieces, axis=0).astype(BF)
        out_ref[:, :, block * 384 : block * 384 + 384] = (
            lax.dot_general(pick, stacked, NT, preferred_element_type=F32)
            .astype(BF)
            .reshape(ROWS, 2, 384)
        )


def body(n_chips, tokens, w_upper, w_surface, bias):
    t = jnp.transpose(tokens, (0, 1, 3, 2, 4))
    width = t.shape[-1]
    vmem = pl.BlockSpec(memory_space=pltpu.VMEM)
    smem = pl.BlockSpec(memory_space=pltpu.SMEM)
    hbm = pl.BlockSpec(memory_space=pl.ANY)
    dma = pltpu.SemaphoreType.DMA
    rows = pl.pallas_call(
        functools.partial(kernel, n_chips),
        out_shape=jax.ShapeDtypeStruct((ROWS, 2, n_chips * 24), BF),
        in_specs=[hbm, hbm, hbm, smem],
        out_specs=vmem,
        scratch_shapes=[
            pltpu.VMEM((n_chips, 7, 8, 128), BF),
            pltpu.VMEM((n_chips, 4, 8, 128), BF),
            pltpu.VMEM(t.shape, BF),
            pltpu.VMEM(w_upper.shape, BF),
            pltpu.VMEM(w_surface.shape, BF),
            pltpu.VMEM((640, 3 * width), BF),
            pltpu.VMEM((320, 2 * width), BF),
            pltpu.VMEM((320, 2 * width), BF),
            pltpu.VMEM((256, 3 * width), BF),
            pltpu.VMEM((128, 2 * width), BF),
            pltpu.VMEM((128, 2 * width), BF),
            pltpu.VMEM((LAT, LAT), BF),
            pltpu.VMEM((640, 256), F32),
            pltpu.VMEM((320, 256), F32),
            dma((t.shape[1] + 2,)),
            pltpu.VMEM((TILES, 3, 8, 128), F32),
            pltpu.VMEM((TILES, 8, 128), BF),
            pltpu.VMEM((2, TILES, 8, 128), BF),
            pltpu.VMEM((n_chips, 7, 8, 128), BF),
            dma((2,)),
            dma((2,)),
            dma((n_chips,)),
            dma((n_chips,)),
            dma((n_chips // SIDE,)),
            dma((n_chips // SIDE,)),
        ],
        compiler_params=pltpu.CompilerParams(
            collective_id=0, has_side_effects=True, vmem_limit_bytes=64 * 10**6
        ),
        name="recover",
    )(t, w_upper, w_surface, bias)
    return jnp.transpose(rows, (1, 0, 2))


def solution(mesh):
    n_chips = mesh.shape["win"] // 2
    return jax.shard_map(
        functools.partial(body, n_chips),
        mesh=mesh,
        in_specs=(P("grp", None, None, "win", None), P(), P(), P()),
        out_specs=P("grp", "win", None),
        check_vma=False,
    )
```

```python
import functools

import jax
import jax.numpy as jnp
from jax import lax
from jax.experimental import pallas as pl
from jax.experimental.pallas import tpu as pltpu
from jax.sharding import PartitionSpec as P

MESH = pl.DeviceIdType.MESH
BF = jnp.bfloat16
F32 = jnp.float32
VARS_UP = 5
LEVELS = 13
VARS_SF = 4
CHANNELS = VARS_UP * LEVELS + VARS_SF
LAT = 256
ROWS = CHANNELS * LAT // 128
TILES = ROWS + 2
NT = (((1,), (1,)), ((), ()))
SIDE = 8


def step_of(dy, dx):
    return ((dy - dx + SIDE) % SIDE) * SIDE + dx


def offset_of(s):
    dx = s % SIDE
    return (s // SIDE + dx) % SIDE, dx


def prepare(w_ref, kinds, last_ref, first_ref, rims_ref):
    width = w_ref.shape[0]
    row = lax.broadcasted_iota(jnp.int32, (8, width), 0)
    a = lax.broadcasted_iota(jnp.int32, (128, 128), 0)
    b = lax.broadcasted_iota(jnp.int32, (128, 128), 1)
    unit = jnp.where(a == b, 1.0, 0.0).astype(BF)

    def keep(mask, value):
        return jnp.where(mask, value, 0.0)

    turned = [
        lax.dot_general(unit, w_ref[:, i * 128 : i * 128 + 128], NT, preferred_element_type=F32)
        for i in range(kinds // 2)
    ]
    for pair in range(kinds // 2):
        for lat in range(8):
            eights = [turned[pair][k * 64 + lat * 8 : k * 64 + lat * 8 + 8] for k in range(2)]
            across = [pltpu.roll(e, 4, 0) for e in eights]
            down = [pltpu.roll(e, 2, 0) for e in eights]
            up = [pltpu.roll(e, 6, 0) for e in eights]
            at = (lat * kinds + 2 * pair) * 8
            for j, parts in enumerate(
                (
                    [keep(row < 4, e) for e in across],
                    eights,
                    [keep(row >= 4, e) for e in across],
                )
            ):
                both = jnp.concatenate(parts, axis=0)
                last_ref[at : at + 16, j * width : (j + 1) * width] = both.astype(BF)
            half = at // 2
            middle = jnp.where(row < 4, up[0], down[1])
            first_ref[half : half + 8, :width] = keep(row % 4 < 2, middle).astype(BF)
            first_ref[half : half + 8, width:] = keep(row % 4 >= 2, middle).astype(BF)
            outer = keep((row == 2) | (row == 3), down[0]) + keep(row >= 6, up[1])
            tail = keep(row < 2, down[0]) + keep((row == 4) | (row == 5), up[1])
            rims_ref[half : half + 8, :width] = outer.astype(BF)
            rims_ref[half : half + 8, width:] = tail.astype(BF)


def latitude(product_ref, rows, lane0):
    place = lax.broadcasted_iota(jnp.int32, (rows, 128), 1)
    lane = place % 64
    parts = []
    for b in range(4):
        main = product_ref[(b + 2) * rows : (b + 3) * rows, lane0 : lane0 + 128]
        a = (b + 6) % 8
        other = product_ref[a * rows : (a + 1) * rows, lane0 : lane0 + 128]
        if b < 2:
            moved = jnp.where(lane != 0, pltpu.roll(other, 1, 1), 0.0)
        else:
            moved = jnp.where(lane != 63, pltpu.roll(other, 127, 1), 0.0)
        parts.append(main + moved)
    low = place < 64
    turned = [pltpu.roll(p, 64, 1) for p in parts]
    return [
        jnp.concatenate(
            [jnp.where(low, parts[0], turned[1]), jnp.where(low, parts[2], turned[3])], axis=1
        ),
        jnp.concatenate(
            [jnp.where(low, turned[0], parts[1]), jnp.where(low, turned[2], parts[3])], axis=1
        ),
    ]


def kernel(
    n_chips,
    t_ref,
    wu_any,
    ws_any,
    bias_ref,
    got_ref,
    twin_ref,
    held,
    wu_ref,
    ws_ref,
    ua_ref,
    ub_ref,
    ur_ref,
    sa_ref,
    sb_ref,
    sr_ref,
    perm_ref,
    prod_a,
    prod_b,
    token_sem,
    image,
    rim_out,
    rim_in,
    chunks,
    rim_send,
    rim_recv,
    own_sem,
    send_sem,
    recv_sem,
    twin_send,
    twin_recv,
):
    n_win = 2 * n_chips
    w = lax.axis_index("win")
    chip, core = w // 2, w % 2
    y, x = chip // SIDE, chip % SIDE
    twin = chip * 2 + 1 - core
    right, left = (w + 1) % n_win, (w + n_win - 1) % n_win
    across = jnp.where(core == 1, right, left)

    levels = t_ref.shape[1]
    pairs = levels // 2

    def token_copy(z):
        return pltpu.make_async_copy(t_ref.at[:, z], held.at[:, z], token_sem.at[z])

    weight_copies = [
        pltpu.make_async_copy(wu_any, wu_ref, token_sem.at[levels]),
        pltpu.make_async_copy(ws_any, ws_ref, token_sem.at[levels + 1]),
    ]
    for copy in weight_copies:
        copy.start()
    for z in range(levels - 1, -1, -1):
        token_copy(z).start()

    barrier = pltpu.get_barrier_semaphore()

    def greet(s, _):
        other = ((chip + s) % n_chips) * 2 + core
        pl.semaphore_signal(barrier, 1, device_id={"win": other}, device_id_type=MESH)
        return 0

    lax.fori_loop(1, n_chips, greet, 0)
    pl.semaphore_signal(barrier, 1, device_id={"win": twin}, device_id_type=MESH)
    pl.semaphore_signal(barrier, 1, device_id={"win": across}, device_id_type=MESH)

    k256 = lax.broadcasted_iota(jnp.int32, (LAT, LAT), 0)
    n256 = lax.broadcasted_iota(jnp.int32, (LAT, LAT), 1)
    perm_ref[...] = jnp.where(4 * (k256 % 64) + k256 // 64 == n256, 1.0, 0.0).astype(BF)
    weight_copies[0].wait()
    prepare(wu_ref, 2 * VARS_UP, ua_ref, ub_ref, ur_ref)
    weight_copies[1].wait()
    prepare(ws_ref, VARS_SF, sa_ref, sb_ref, sr_ref)

    row8 = lax.broadcasted_iota(jnp.int32, (8, 128), 0)
    low4 = row8 % 4 < 2

    def columns(zs, j):
        return jnp.concatenate([held[m, z, j] for z in zs for m in range(2)], axis=0)

    def halves(values, at):
        for h in range(2):
            first = values[0][at : at + 8, h * 128 : h * 128 + 128]
            second = values[1][at : at + 8, h * 128 : h * 128 + 128]
            yield h, jnp.where(row8 < 4, first, pltpu.roll(second, 4, 0)), jnp.where(
                row8 < 4, pltpu.roll(first, 4, 0), second
            )

    def interleaved(blocks):
        stacked = jnp.concatenate([b.astype(BF) for b in blocks], axis=0)
        value = jnp.dot(stacked, perm_ref[...], preferred_element_type=F32)
        out, at = [], 0
        for b in blocks:
            out.append(value[at : at + b.shape[0]])
            at += b.shape[0]
        return out

    def per_member(product_ref, rows, count):
        found = [latitude(product_ref, rows, zi * 128) for zi in range(count)]
        return [jnp.concatenate([f[m] for f in found], axis=0) for m in range(2)]

    def rims(zs, w_ref, kinds, channel):
        rhs = jnp.concatenate([columns(zs, 0), columns(zs, 2)], axis=1)
        n = rhs.shape[0]
        rows = kinds * 4
        prod_b[: 8 * rows, :n] = lax.dot_general(w_ref[...], rhs, NT, preferred_element_type=F32)
        values = interleaved(per_member(prod_b, rows, len(zs)))
        for zi in range(len(zs)):
            for v in range(kinds // 2):
                c0, c1 = channel(zi, 2 * v), channel(zi, 2 * v + 1)
                (_, one0, two0), (_, one1, two1) = halves(values, zi * rows + 8 * v)
                for c, first, second in ((c0, one0, one1), (c1, two0, two1)):
                    rim_out[0, c] = jnp.where(low4, first, pltpu.roll(second, 2, 0)).astype(BF)
                    rim_out[1, c] = jnp.where(low4, pltpu.roll(first, 6, 0), second).astype(BF)

    def inner(zs, a_ref, b_ref, kinds, channel):
        three = [columns(zs, j) for j in range(3)]
        rhs = jnp.concatenate(three, axis=1)
        n = rhs.shape[0]
        rows_a, rows_b = kinds * 8, kinds * 4
        prod_a[: 8 * rows_a, :n] = lax.dot_general(a_ref[...], rhs, NT, preferred_element_type=F32)
        rhs = jnp.concatenate([three[0], three[2]], axis=1)
        prod_b[: 8 * rows_b, :n] = lax.dot_general(b_ref[...], rhs, NT, preferred_element_type=F32)
        values = interleaved(
            per_member(prod_a, rows_a, len(zs)) + per_member(prod_b, rows_b, len(zs))
        )
        for zi in range(len(zs)):
            for k in range(kinds):
                c = channel(zi, k)
                at = zi * rows_a + 8 * k
                for m in range(2):
                    for h in range(2):
                        lo = h * 128
                        image[2 * c + h, m] = values[m][at : at + 8, lo : lo + 128] + bias_ref[c]
            for v in range(kinds // 2):
                c0, c1 = channel(zi, 2 * v), channel(zi, 2 * v + 1)
                for h, one, two in halves(values[2:], zi * rows_b + 8 * v):
                    image[2 * c0 + h, 2] = one + bias_ref[c0]
                    image[2 * c1 + h, 2] = two + bias_ref[c1]

    def upper_rims(q, _):
        p = pairs - 1 - q
        token_copy(2 * p + 1).wait()
        token_copy(2 * p).wait()
        rims((2 * p, 2 * p + 1), ur_ref, 10, lambda zi, k: 13 * (k // 2) + 2 * (2 * p + zi) + k % 2)
        return 0

    def upper_inner(q, _):
        p = pairs - 1 - q
        inner(
            (2 * p, 2 * p + 1),
            ua_ref,
            ub_ref,
            10,
            lambda zi, k: 13 * (k // 2) + 2 * (2 * p + zi) + k % 2,
        )
        return 0

    def surface_channel(zi, k):
        return VARS_UP * LEVELS + k

    lax.fori_loop(0, pairs, upper_rims, 0)
    rims((levels - 1,), sr_ref, 4, surface_channel)

    lane = lax.broadcasted_iota(jnp.int32, (8, 128), 1)
    parts = (pl.ds(0, 4), pl.ds(4, 3))

    def target(s):
        dy, dx = offset_of(s)
        return ((y + dy) % SIDE) * SIDE + (x + dx) % SIDE

    def send_copy(half, s):
        return pltpu.make_async_remote_copy(
            src_ref=chunks.at[s, parts[half]],
            dst_ref=got_ref.at[s, parts[half]],
            send_sem=send_sem.at[half, s],
            recv_sem=recv_sem.at[half, s],
            device_id={"win": target(s) * 2 + core},
            device_id_type=MESH,
        )

    def window(to, k):
        d = to * 2 + k
        o = (d * ROWS) % 128
        return (d * ROWS) // 128, o, (128 - o) % 128

    def first_part(s):
        to = target(s)
        for k in range(2):
            t, o, back = window(to, k)
            for g in range(2):
                a = pltpu.roll(image[t, g], back, 1)
                b = pltpu.roll(image[t + 1, g], back, 1)
                chunks[s, 2 * k + g] = jnp.where(lane < 128 - o, a, b).astype(BF)

    def second_part(s):
        to = target(s)
        tails = jnp.zeros((8, 128), F32)
        for k in range(2):
            t, o, back = window(to, k)
            a = pltpu.roll(image[t, 2], back, 1)
            b = pltpu.roll(image[t + 1, 2], back, 1)
            chunks[s, 4 + 2 * k] = jnp.where(lane < 128 - o, a, b).astype(BF)
            for slot, g in enumerate((0, 1, 2, 2)):
                at = 64 * k + 16 * slot
                b = pltpu.roll(image[t + 1, g], (back + at) % 128, 1)
                c = pltpu.roll(image[t + 2, g], (back + at) % 128, 1)
                tail = jnp.where(lane < 128 - o + at, b, c)
                tails = jnp.where((lane >= at) & (lane < at + 10), tail, tails)
        chunks[s, 5] = tails.astype(BF)

    def own_copy(half):
        return pltpu.make_async_copy(
            chunks.at[0, parts[half]], got_ref.at[0, parts[half]], own_sem.at[half]
        )

    def all_inner():
        lax.fori_loop(0, pairs, upper_inner, 0)
        inner((levels - 1,), sa_ref, sb_ref, 4, surface_channel)

    late = (y >= SIDE // 2) | (chip == 0)
    def early_inner():
        all_inner()

        def cut(q, _):
            for u in range(4):
                first_part(q * 4 + u)
            return 0

        lax.fori_loop(0, n_chips // 4, cut, 0)

    pl.when(jnp.logical_not(late))(early_inner)
    pl.semaphore_wait(barrier, n_chips + 1)
    rim_copies = []
    for side, other in ((0, right), (1, left)):
        copy = pltpu.make_async_remote_copy(
            src_ref=rim_out.at[side],
            dst_ref=rim_in.at[side],
            send_sem=rim_send.at[side],
            recv_sem=rim_recv.at[side],
            device_id={"win": other},
            device_id_type=MESH,
        )
        copy.start()
        rim_copies.append(copy)

    def late_inner():
        all_inner()

        def cut_and_send(q, _):
            for u in range(7):
                first_part(1 + q * 7 + u)
            for u in range(7):
                send_copy(0, 1 + q * 7 + u).start()
            return 0

        lax.fori_loop(0, (n_chips - 1) // 7, cut_and_send, 0)
        first_part(0)

    def early_send():
        def send_first(s, _):
            send_copy(0, s).start()
            return 0

        lax.fori_loop(1, n_chips, send_first, 0)

    pl.when(late)(late_inner)
    pl.when(jnp.logical_not(late))(early_send)
    own_copy(0).start()


    for copy in rim_copies:
        copy.wait()

    def add_rims(q, _):
        for u in range(3):
            c = q * 3 + u
            before = rim_in[0, c].astype(F32)
            after = rim_in[1, c].astype(F32)
            image[2 * c, 2] += jnp.where(low4, before, pltpu.roll(after, 2, 0))
            image[2 * c + 1, 2] += jnp.where(low4, pltpu.roll(before, 6, 0), after)
        return 0

    lax.fori_loop(0, CHANNELS // 3, add_rims, 0)

    def send_second(q, _):
        for u in range(7):
            second_part(1 + q * 7 + u)
        for u in range(7):
            send_copy(1, 1 + q * 7 + u).start()
        return 0

    lax.fori_loop(0, (n_chips - 1) // 7, send_second, 0)
    second_part(0)
    own_copy(1).start()
    for half in range(2):
        own_copy(half).wait()

    def twin_copy(half, g):
        chips = pl.ds(g * SIDE, SIDE)
        first = (2 * (1 - core), 4 + 1 - core)[half]
        return pltpu.make_async_remote_copy(
            src_ref=got_ref.at[chips, pl.ds(first, 2)],
            dst_ref=twin_ref.at[chips, pl.ds(2 * half, 2)],
            send_sem=twin_send.at[half, g],
            recv_sem=twin_recv.at[half, g],
            device_id={"win": twin},
            device_id_type=MESH,
        )

    for half in range(2):

        def arrived(s, _):
            send_copy(half, s).wait_recv()
            return 0

        for g in range(n_chips // SIDE):
            lax.fori_loop(max(1, g * SIDE), (g + 1) * SIDE, arrived, 0)
            twin_copy(half, g).start()

    for half in range(2):

        def left_here(s, _):
            send_copy(half, s).wait_send()
            return 0

        lax.fori_loop(1, n_chips, left_here, 0)
        for g in range(n_chips // SIDE):
            twin_copy(half, g).wait()


def finish(n_chips, got_any, twin_any, out_any, got_ref, twin_ref, rows_ref, in_sem, out_sem):
    w = lax.axis_index("win")
    chip, core = w // 2, w % 2
    y, x = chip // SIDE, chip % SIDE
    loads = [
        pltpu.make_async_copy(twin_any, twin_ref, in_sem.at[0]),
        pltpu.make_async_copy(
            got_any.at[:, pl.ds(2 * core, 2)], got_ref.at[:, pl.ds(0, 2)], in_sem.at[1]
        ),
        pltpu.make_async_copy(
            got_any.at[:, pl.ds(4 + core, 2)], got_ref.at[:, pl.ds(2, 2)], in_sem.at[2]
        ),
    ]
    for load in loads:
        load.start()
    first = core == 0
    row = lax.broadcasted_iota(jnp.int32, (8, 128), 0)
    lane = lax.broadcasted_iota(jnp.int32, (8, 128), 1)
    spot = lane - 64 * core
    bands = ((spot >= 0) & (spot < 10)) | ((spot >= 16) & (spot < 26))
    third = (spot >= 32) & (spot < 42)
    fourth = (spot >= 48) & (spot < 58)

    def select(mask, value):
        return jnp.where(mask, value, 0.0)

    def ordered(ga, gb, ra, rb):
        middle = jnp.where(row < 4, ga, jnp.where(row < 6, gb, rb))
        return jnp.concatenate(
            [jnp.where(row < 2, ga, ra), jnp.where(row < 2, ra, middle), jnp.where(row < 6, rb, gb)],
            axis=0,
        )

    r = lax.broadcasted_iota(jnp.int32, (2 * ROWS, 384), 0)
    k = lax.broadcasted_iota(jnp.int32, (2 * ROWS, 384), 1)
    rho, m = r // 2, r % 2
    at = 256 + 64 * core + 16 * m + rho - 128
    hot = ((rho < 128) & (k == 128 * m + rho)) | ((rho >= 128) & ((k == at) | (k == at + 32)))
    pick = jnp.where(hot, 1.0, 0.0).astype(BF)
    for load in loads:
        load.wait()

    def out_copy(block):
        part = pl.ds(block * 384, 384)
        return pltpu.make_async_copy(
            rows_ref.at[:, :, part], out_any.at[:, :, part], out_sem.at[block]
        )

    for block in range(n_chips // 16):
        pieces = []
        for i in range(16):
            p = block * 16 + i
            s = step_of((y - p // SIDE + SIDE) % SIDE, (x - p % SIDE + SIDE) % SIDE)
            mine = [got_ref[s, u].astype(F32) for u in range(4)]
            other = [twin_ref[s, u].astype(F32) for u in range(4)]
            a, b = [], []
            for u in (0, 1, 2, 3):
                v = u if u < 2 else 5 - u
                here = jnp.where(first, mine[u], mine[v])
                there = jnp.where(first, other[u], other[v])
                a.append(jnp.where(first, here, there))
                b.append(jnp.where(first, there, here))
            ga, gb = pltpu.roll(a[2], 4, 0), pltpu.roll(b[2], 4, 0)
            ta, tb = pltpu.roll(a[3], 4, 0), pltpu.roll(b[3], 4, 0)
            blocks = [
                ordered(a[2], gb, pltpu.roll(a[0], 2, 0), pltpu.roll(b[0], 6, 0)),
                ordered(ga, b[2], pltpu.roll(a[1], 2, 0), pltpu.roll(b[1], 6, 0)),
                ordered(
                    select(third, a[3]) + select(fourth, ta),
                    select(third, tb) + select(fourth, b[3]),
                    select(bands, pltpu.roll(a[3], 2, 0)),
                    select(bands, pltpu.roll(b[3], 6, 0)),
                ),
            ]
            pieces.append(jnp.concatenate(blocks, axis=1))
        stacked = jnp.concatenate(pieces, axis=0).astype(BF)
        rows_ref[:, :, block * 384 : block * 384 + 384] = (
            lax.dot_general(pick, stacked, NT, preferred_element_type=F32)
            .astype(BF)
            .reshape(ROWS, 2, 384)
        )
        out_copy(block).start()
    for block in range(n_chips // 16):
        out_copy(block).wait()


def body(n_chips, tokens, w_upper, w_surface, bias):
    t = jnp.transpose(tokens, (0, 1, 3, 2, 4))
    width = t.shape[-1]
    smem = pl.BlockSpec(memory_space=pltpu.SMEM)
    hbm = pl.BlockSpec(memory_space=pl.ANY)
    dma = pltpu.SemaphoreType.DMA
    got, twin = pl.pallas_call(
        functools.partial(kernel, n_chips),
        out_shape=(
            jax.ShapeDtypeStruct((n_chips, 7, 8, 128), BF),
            jax.ShapeDtypeStruct((n_chips, 4, 8, 128), BF),
        ),
        in_specs=[hbm, hbm, hbm, smem],
        out_specs=(hbm, hbm),
        scratch_shapes=[
            pltpu.VMEM(t.shape, BF),
            pltpu.VMEM(w_upper.shape, BF),
            pltpu.VMEM(w_surface.shape, BF),
            pltpu.VMEM((640, 3 * width), BF),
            pltpu.VMEM((320, 2 * width), BF),
            pltpu.VMEM((320, 2 * width), BF),
            pltpu.VMEM((256, 3 * width), BF),
            pltpu.VMEM((128, 2 * width), BF),
            pltpu.VMEM((128, 2 * width), BF),
            pltpu.VMEM((LAT, LAT), BF),
            pltpu.VMEM((640, 256), F32),
            pltpu.VMEM((320, 256), F32),
            dma((t.shape[1] + 2,)),
            pltpu.VMEM((TILES, 3, 8, 128), F32),
            pltpu.VMEM((2, CHANNELS, 8, 128), BF),
            pltpu.VMEM((2, CHANNELS, 8, 128), BF),
            pltpu.VMEM((n_chips, 7, 8, 128), BF),
            dma((2,)),
            dma((2,)),
            dma((2,)),
            dma((2, n_chips)),
            dma((2, n_chips)),
            dma((2, n_chips // SIDE)),
            dma((2, n_chips // SIDE)),
        ],
        compiler_params=pltpu.CompilerParams(
            collective_id=0, has_side_effects=True, vmem_limit_bytes=64 * 10**6
        ),
        name="recover",
    )(t, w_upper, w_surface, bias)
    rows = pl.pallas_call(
        functools.partial(finish, n_chips),
        out_shape=jax.ShapeDtypeStruct((ROWS, 2, n_chips * 24), BF),
        in_specs=[hbm, hbm],
        out_specs=hbm,
        scratch_shapes=[
            pltpu.VMEM((n_chips, 4, 8, 128), BF),
            pltpu.VMEM((n_chips, 4, 8, 128), BF),
            pltpu.VMEM((ROWS, 2, n_chips * 24), BF),
            dma((3,)),
            dma((n_chips // 16,)),
        ],
        compiler_params=pltpu.CompilerParams(vmem_limit_bytes=64 * 10**6),
        name="finish",
    )(got, twin)
    return jnp.transpose(rows, (1, 0, 2))


def solution(mesh):
    n_chips = mesh.shape["win"] // 2
    return jax.shard_map(
        functools.partial(body, n_chips),
        mesh=mesh,
        in_specs=(P("grp", None, None, "win", None), P(), P(), P()),
        out_specs=P("grp", "win", None),
        check_vma=False,
    )
```

```python
import functools

import jax
import jax.numpy as jnp
from jax import lax
from jax.experimental import pallas as pl
from jax.experimental.pallas import tpu as pltpu
from jax.sharding import PartitionSpec as P

MESH = pl.DeviceIdType.MESH
BF = jnp.bfloat16
F32 = jnp.float32
VARS_UP = 5
LEVELS = 13
VARS_SF = 4
CHANNELS = VARS_UP * LEVELS + VARS_SF
LAT = 256
ROWS = CHANNELS * LAT // 128
TILES = ROWS + 2
NT = (((1,), (1,)), ((), ()))
SIDE = 8


def step_of(dy, dx):
    return ((dy - dx + SIDE) % SIDE) * SIDE + dx


def offset_of(s):
    dx = s % SIDE
    return (s // SIDE + dx) % SIDE, dx


def prepare(w_ref, kinds, last_ref, first_ref, rims_ref):
    width = w_ref.shape[0]
    row = lax.broadcasted_iota(jnp.int32, (8, width), 0)
    a = lax.broadcasted_iota(jnp.int32, (128, 128), 0)
    b = lax.broadcasted_iota(jnp.int32, (128, 128), 1)
    unit = jnp.where(a == b, 1.0, 0.0).astype(BF)

    def keep(mask, value):
        return jnp.where(mask, value, 0.0)

    turned = [
        lax.dot_general(unit, w_ref[:, i * 128 : i * 128 + 128], NT, preferred_element_type=F32)
        for i in range(kinds // 2)
    ]
    for pair in range(kinds // 2):
        for lat in range(8):
            eights = [turned[pair][k * 64 + lat * 8 : k * 64 + lat * 8 + 8] for k in range(2)]
            across = [pltpu.roll(e, 4, 0) for e in eights]
            down = [pltpu.roll(e, 2, 0) for e in eights]
            up = [pltpu.roll(e, 6, 0) for e in eights]
            at = (lat * kinds + 2 * pair) * 8
            for j, parts in enumerate(
                (
                    [keep(row < 4, e) for e in across],
                    eights,
                    [keep(row >= 4, e) for e in across],
                )
            ):
                both = jnp.concatenate(parts, axis=0)
                last_ref[at : at + 16, j * width : (j + 1) * width] = both.astype(BF)
            half = at // 2
            middle = jnp.where(row < 4, up[0], down[1])
            first_ref[half : half + 8, :width] = keep(row % 4 < 2, middle).astype(BF)
            first_ref[half : half + 8, width:] = keep(row % 4 >= 2, middle).astype(BF)
            outer = keep((row == 2) | (row == 3), down[0]) + keep(row >= 6, up[1])
            tail = keep(row < 2, down[0]) + keep((row == 4) | (row == 5), up[1])
            rims_ref[half : half + 8, :width] = outer.astype(BF)
            rims_ref[half : half + 8, width:] = tail.astype(BF)


def latitude(product_ref, rows, lane0):
    place = lax.broadcasted_iota(jnp.int32, (rows, 128), 1)
    lane = place % 64
    parts = []
    for b in range(4):
        main = product_ref[(b + 2) * rows : (b + 3) * rows, lane0 : lane0 + 128]
        a = (b + 6) % 8
        other = product_ref[a * rows : (a + 1) * rows, lane0 : lane0 + 128]
        if b < 2:
            moved = jnp.where(lane != 0, pltpu.roll(other, 1, 1), 0.0)
        else:
            moved = jnp.where(lane != 63, pltpu.roll(other, 127, 1), 0.0)
        parts.append(main + moved)
    low = place < 64
    turned = [pltpu.roll(p, 64, 1) for p in parts]
    return [
        jnp.concatenate(
            [jnp.where(low, parts[0], turned[1]), jnp.where(low, parts[2], turned[3])], axis=1
        ),
        jnp.concatenate(
            [jnp.where(low, turned[0], parts[1]), jnp.where(low, turned[2], parts[3])], axis=1
        ),
    ]


def kernel(
    n_chips,
    t_ref,
    wu_any,
    ws_any,
    bias_ref,
    got_ref,
    twin_ref,
    held,
    wu_ref,
    ws_ref,
    ua_ref,
    ub_ref,
    ur_ref,
    sa_ref,
    sb_ref,
    sr_ref,
    perm_ref,
    prod_a,
    prod_b,
    token_sem,
    image,
    rim_out,
    rim_in,
    chunks,
    rim_send,
    rim_recv,
    own_sem,
    send_sem,
    recv_sem,
    twin_send,
    twin_recv,
):
    n_win = 2 * n_chips
    w = lax.axis_index("win")
    chip, core = w // 2, w % 2
    y, x = chip // SIDE, chip % SIDE
    twin = chip * 2 + 1 - core
    right, left = (w + 1) % n_win, (w + n_win - 1) % n_win
    across = jnp.where(core == 1, right, left)

    levels = t_ref.shape[1]
    pairs = levels // 2

    def token_copy(z):
        return pltpu.make_async_copy(t_ref.at[:, z], held.at[:, z], token_sem.at[z])

    weight_copies = [
        pltpu.make_async_copy(wu_any, wu_ref, token_sem.at[levels]),
        pltpu.make_async_copy(ws_any, ws_ref, token_sem.at[levels + 1]),
    ]
    for copy in weight_copies:
        copy.start()
    for z in range(levels - 1, -1, -1):
        token_copy(z).start()

    barrier = pltpu.get_barrier_semaphore()

    def greet(s, _):
        other = ((chip + s) % n_chips) * 2 + core
        pl.semaphore_signal(barrier, 1, device_id={"win": other}, device_id_type=MESH)
        return 0

    lax.fori_loop(1, n_chips, greet, 0)
    pl.semaphore_signal(barrier, 1, device_id={"win": twin}, device_id_type=MESH)
    pl.semaphore_signal(barrier, 1, device_id={"win": across}, device_id_type=MESH)

    k256 = lax.broadcasted_iota(jnp.int32, (LAT, LAT), 0)
    n256 = lax.broadcasted_iota(jnp.int32, (LAT, LAT), 1)
    perm_ref[...] = jnp.where(4 * (k256 % 64) + k256 // 64 == n256, 1.0, 0.0).astype(BF)
    weight_copies[0].wait()
    prepare(wu_ref, 2 * VARS_UP, ua_ref, ub_ref, ur_ref)
    weight_copies[1].wait()
    prepare(ws_ref, VARS_SF, sa_ref, sb_ref, sr_ref)

    row8 = lax.broadcasted_iota(jnp.int32, (8, 128), 0)
    low4 = row8 % 4 < 2

    def columns(zs, j):
        return jnp.concatenate([held[m, z, j] for z in zs for m in range(2)], axis=0)

    def halves(values, at):
        for h in range(2):
            first = values[0][at : at + 8, h * 128 : h * 128 + 128]
            second = values[1][at : at + 8, h * 128 : h * 128 + 128]
            yield h, jnp.where(row8 < 4, first, pltpu.roll(second, 4, 0)), jnp.where(
                row8 < 4, pltpu.roll(first, 4, 0), second
            )

    def interleaved(blocks):
        stacked = jnp.concatenate([b.astype(BF) for b in blocks], axis=0)
        value = jnp.dot(stacked, perm_ref[...], preferred_element_type=F32)
        out, at = [], 0
        for b in blocks:
            out.append(value[at : at + b.shape[0]])
            at += b.shape[0]
        return out

    def per_member(product_ref, rows, count):
        found = [latitude(product_ref, rows, zi * 128) for zi in range(count)]
        return [jnp.concatenate([f[m] for f in found], axis=0) for m in range(2)]

    def rims(zs, w_ref, kinds, channel):
        rhs = jnp.concatenate([columns(zs, 0), columns(zs, 2)], axis=1)
        n = rhs.shape[0]
        rows = kinds * 4
        prod_b[: 8 * rows, :n] = lax.dot_general(w_ref[...], rhs, NT, preferred_element_type=F32)
        values = interleaved(per_member(prod_b, rows, len(zs)))
        for zi in range(len(zs)):
            for v in range(kinds // 2):
                c0, c1 = channel(zi, 2 * v), channel(zi, 2 * v + 1)
                (_, one0, two0), (_, one1, two1) = halves(values, zi * rows + 8 * v)
                for c, first, second in ((c0, one0, one1), (c1, two0, two1)):
                    rim_out[0, c] = jnp.where(low4, first, pltpu.roll(second, 2, 0)).astype(BF)
                    rim_out[1, c] = jnp.where(low4, pltpu.roll(first, 6, 0), second).astype(BF)

    def inner(zs, w_ref, kinds, channel):
        rhs = jnp.concatenate([columns(zs, j) for j in range(3)], axis=1)
        n = rhs.shape[0]
        rows = kinds * 8
        prod_a[: 8 * rows, :n] = lax.dot_general(w_ref[...], rhs, NT, preferred_element_type=F32)
        values = interleaved(per_member(prod_a, rows, len(zs)))
        for zi in range(len(zs)):
            for k in range(kinds):
                c = channel(zi, k)
                at = zi * rows + 8 * k
                for m in range(2):
                    for h in range(2):
                        lo = h * 128
                        image[2 * c + h, m] = values[m][at : at + 8, lo : lo + 128] + bias_ref[c]

    def outer(zs, w_ref, kinds, channel):
        rhs = jnp.concatenate([columns(zs, 0), columns(zs, 2)], axis=1)
        n = rhs.shape[0]
        rows = kinds * 4
        prod_b[: 8 * rows, :n] = lax.dot_general(w_ref[...], rhs, NT, preferred_element_type=F32)
        values = interleaved(per_member(prod_b, rows, len(zs)))
        for zi in range(len(zs)):
            for v in range(kinds // 2):
                c0, c1 = channel(zi, 2 * v), channel(zi, 2 * v + 1)
                for h, one, two in halves(values, zi * rows + 8 * v):
                    image[2 * c0 + h, 2] = one + bias_ref[c0]
                    image[2 * c1 + h, 2] = two + bias_ref[c1]

    def upper_rims(q, _):
        p = pairs - 1 - q
        token_copy(2 * p + 1).wait()
        token_copy(2 * p).wait()
        rims((2 * p, 2 * p + 1), ur_ref, 10, lambda zi, k: 13 * (k // 2) + 2 * (2 * p + zi) + k % 2)
        return 0

    def upper_channel(p):
        return lambda zi, k: 13 * (k // 2) + 2 * (2 * p + zi) + k % 2

    def upper_inner(q, _):
        p = pairs - 1 - q
        inner((2 * p, 2 * p + 1), ua_ref, 10, upper_channel(p))
        return 0

    def upper_outer(q, _):
        p = pairs - 1 - q
        outer((2 * p, 2 * p + 1), ub_ref, 10, upper_channel(p))
        return 0

    def surface_channel(zi, k):
        return VARS_UP * LEVELS + k

    lax.fori_loop(0, pairs, upper_rims, 0)
    rims((levels - 1,), sr_ref, 4, surface_channel)

    lane = lax.broadcasted_iota(jnp.int32, (8, 128), 1)
    parts = (pl.ds(0, 4), pl.ds(4, 3))

    def target(s):
        dy, dx = offset_of(s)
        return ((y + dy) % SIDE) * SIDE + (x + dx) % SIDE

    def send_copy(half, s):
        return pltpu.make_async_remote_copy(
            src_ref=chunks.at[s, parts[half]],
            dst_ref=got_ref.at[s, parts[half]],
            send_sem=send_sem.at[half, s],
            recv_sem=recv_sem.at[half, s],
            device_id={"win": target(s) * 2 + core},
            device_id_type=MESH,
        )

    def window(to, k):
        d = to * 2 + k
        o = (d * ROWS) % 128
        return (d * ROWS) // 128, o, (128 - o) % 128

    def first_part(s):
        to = target(s)
        for k in range(2):
            t, o, back = window(to, k)
            for g in range(2):
                a = pltpu.roll(image[t, g], back, 1)
                b = pltpu.roll(image[t + 1, g], back, 1)
                chunks[s, 2 * k + g] = jnp.where(lane < 128 - o, a, b).astype(BF)

    def second_part(s):
        to = target(s)
        tails = jnp.zeros((8, 128), F32)
        for k in range(2):
            t, o, back = window(to, k)
            a = pltpu.roll(image[t, 2], back, 1)
            b = pltpu.roll(image[t + 1, 2], back, 1)
            chunks[s, 4 + 2 * k] = jnp.where(lane < 128 - o, a, b).astype(BF)
            for slot, g in enumerate((0, 1, 2, 2)):
                at = 64 * k + 16 * slot
                b = pltpu.roll(image[t + 1, g], (back + at) % 128, 1)
                c = pltpu.roll(image[t + 2, g], (back + at) % 128, 1)
                tail = jnp.where(lane < 128 - o + at, b, c)
                tails = jnp.where((lane >= at) & (lane < at + 10), tail, tails)
        chunks[s, 5] = tails.astype(BF)

    def own_copy(half):
        return pltpu.make_async_copy(
            chunks.at[0, parts[half]], got_ref.at[0, parts[half]], own_sem.at[half]
        )

    def all_inner():
        lax.fori_loop(0, pairs, upper_inner, 0)
        inner((levels - 1,), sa_ref, 4, surface_channel)

    late = (y >= SIDE // 2) | (chip == 0)
    def early_inner():
        all_inner()

        def cut(q, _):
            for u in range(4):
                first_part(q * 4 + u)
            return 0

        lax.fori_loop(0, n_chips // 4, cut, 0)

    pl.when(jnp.logical_not(late))(early_inner)
    pl.semaphore_wait(barrier, n_chips + 1)
    rim_copies = []
    for side, other in ((0, right), (1, left)):
        copy = pltpu.make_async_remote_copy(
            src_ref=rim_out.at[side],
            dst_ref=rim_in.at[side],
            send_sem=rim_send.at[side],
            recv_sem=rim_recv.at[side],
            device_id={"win": other},
            device_id_type=MESH,
        )
        copy.start()
        rim_copies.append(copy)

    def late_inner():
        all_inner()

        def cut_and_send(q, _):
            for u in range(7):
                first_part(1 + q * 7 + u)
            for u in range(7):
                send_copy(0, 1 + q * 7 + u).start()
            return 0

        lax.fori_loop(0, (n_chips - 1) // 7, cut_and_send, 0)
        first_part(0)

    def early_send():
        def send_first(s, _):
            send_copy(0, s).start()
            return 0

        lax.fori_loop(1, n_chips, send_first, 0)

    pl.when(late)(late_inner)
    pl.when(jnp.logical_not(late))(early_send)
    own_copy(0).start()

    lax.fori_loop(0, pairs, upper_outer, 0)
    outer((levels - 1,), sb_ref, 4, surface_channel)


    for copy in rim_copies:
        copy.wait()

    def add_rims(q, _):
        for u in range(3):
            c = q * 3 + u
            before = rim_in[0, c].astype(F32)
            after = rim_in[1, c].astype(F32)
            image[2 * c, 2] += jnp.where(low4, before, pltpu.roll(after, 2, 0))
            image[2 * c + 1, 2] += jnp.where(low4, pltpu.roll(before, 6, 0), after)
        return 0

    lax.fori_loop(0, CHANNELS // 3, add_rims, 0)

    def send_second(q, _):
        for u in range(7):
            second_part(1 + q * 7 + u)
        for u in range(7):
            send_copy(1, 1 + q * 7 + u).start()
        return 0

    lax.fori_loop(0, (n_chips - 1) // 7, send_second, 0)
    second_part(0)
    own_copy(1).start()
    for half in range(2):
        own_copy(half).wait()

    def twin_copy(half, g):
        chips = pl.ds(g * SIDE, SIDE)
        first = (2 * (1 - core), 4 + 1 - core)[half]
        return pltpu.make_async_remote_copy(
            src_ref=got_ref.at[chips, pl.ds(first, 2)],
            dst_ref=twin_ref.at[chips, pl.ds(2 * half, 2)],
            send_sem=twin_send.at[half, g],
            recv_sem=twin_recv.at[half, g],
            device_id={"win": twin},
            device_id_type=MESH,
        )

    for half in range(2):

        def arrived(s, _):
            send_copy(half, s).wait_recv()
            return 0

        for g in range(n_chips // SIDE):
            lax.fori_loop(max(1, g * SIDE), (g + 1) * SIDE, arrived, 0)
            twin_copy(half, g).start()

    for half in range(2):

        def left_here(s, _):
            send_copy(half, s).wait_send()
            return 0

        lax.fori_loop(1, n_chips, left_here, 0)
        for g in range(n_chips // SIDE):
            twin_copy(half, g).wait()


def finish(n_chips, got_any, twin_any, out_any, got_ref, twin_ref, rows_ref, in_sem, out_sem):
    w = lax.axis_index("win")
    chip, core = w // 2, w % 2
    y, x = chip // SIDE, chip % SIDE
    loads = [
        pltpu.make_async_copy(twin_any, twin_ref, in_sem.at[0]),
        pltpu.make_async_copy(
            got_any.at[:, pl.ds(2 * core, 2)], got_ref.at[:, pl.ds(0, 2)], in_sem.at[1]
        ),
        pltpu.make_async_copy(
            got_any.at[:, pl.ds(4 + core, 2)], got_ref.at[:, pl.ds(2, 2)], in_sem.at[2]
        ),
    ]
    for load in loads:
        load.start()
    first = core == 0
    row = lax.broadcasted_iota(jnp.int32, (8, 128), 0)
    lane = lax.broadcasted_iota(jnp.int32, (8, 128), 1)
    spot = lane - 64 * core
    bands = ((spot >= 0) & (spot < 10)) | ((spot >= 16) & (spot < 26))
    third = (spot >= 32) & (spot < 42)
    fourth = (spot >= 48) & (spot < 58)

    def select(mask, value):
        return jnp.where(mask, value, 0.0)

    def ordered(ga, gb, ra, rb):
        middle = jnp.where(row < 4, ga, jnp.where(row < 6, gb, rb))
        return jnp.concatenate(
            [jnp.where(row < 2, ga, ra), jnp.where(row < 2, ra, middle), jnp.where(row < 6, rb, gb)],
            axis=0,
        )

    r = lax.broadcasted_iota(jnp.int32, (2 * ROWS, 384), 0)
    k = lax.broadcasted_iota(jnp.int32, (2 * ROWS, 384), 1)
    rho, m = r // 2, r % 2
    at = 256 + 64 * core + 16 * m + rho - 128
    hot = ((rho < 128) & (k == 128 * m + rho)) | ((rho >= 128) & ((k == at) | (k == at + 32)))
    pick = jnp.where(hot, 1.0, 0.0).astype(BF)
    for load in loads:
        load.wait()

    def out_copy(block):
        part = pl.ds(block * 384, 384)
        return pltpu.make_async_copy(
            rows_ref.at[:, :, part], out_any.at[:, :, part], out_sem.at[block]
        )

    for block in range(n_chips // 16):
        pieces = []
        for i in range(16):
            p = block * 16 + i
            s = step_of((y - p // SIDE + SIDE) % SIDE, (x - p % SIDE + SIDE) % SIDE)
            mine = [got_ref[s, u].astype(F32) for u in range(4)]
            other = [twin_ref[s, u].astype(F32) for u in range(4)]
            a, b = [], []
            for u in (0, 1, 2, 3):
                v = u if u < 2 else 5 - u
                here = jnp.where(first, mine[u], mine[v])
                there = jnp.where(first, other[u], other[v])
                a.append(jnp.where(first, here, there))
                b.append(jnp.where(first, there, here))
            ga, gb = pltpu.roll(a[2], 4, 0), pltpu.roll(b[2], 4, 0)
            ta, tb = pltpu.roll(a[3], 4, 0), pltpu.roll(b[3], 4, 0)
            blocks = [
                ordered(a[2], gb, pltpu.roll(a[0], 2, 0), pltpu.roll(b[0], 6, 0)),
                ordered(ga, b[2], pltpu.roll(a[1], 2, 0), pltpu.roll(b[1], 6, 0)),
                ordered(
                    select(third, a[3]) + select(fourth, ta),
                    select(third, tb) + select(fourth, b[3]),
                    select(bands, pltpu.roll(a[3], 2, 0)),
                    select(bands, pltpu.roll(b[3], 6, 0)),
                ),
            ]
            pieces.append(jnp.concatenate(blocks, axis=1))
        stacked = jnp.concatenate(pieces, axis=0).astype(BF)
        rows_ref[:, :, block * 384 : block * 384 + 384] = (
            lax.dot_general(pick, stacked, NT, preferred_element_type=F32)
            .astype(BF)
            .reshape(ROWS, 2, 384)
        )
        out_copy(block).start()
    for block in range(n_chips // 16):
        out_copy(block).wait()


def body(n_chips, tokens, w_upper, w_surface, bias):
    t = jnp.transpose(tokens, (0, 1, 3, 2, 4))
    width = t.shape[-1]
    smem = pl.BlockSpec(memory_space=pltpu.SMEM)
    hbm = pl.BlockSpec(memory_space=pl.ANY)
    dma = pltpu.SemaphoreType.DMA
    got, twin = pl.pallas_call(
        functools.partial(kernel, n_chips),
        out_shape=(
            jax.ShapeDtypeStruct((n_chips, 7, 8, 128), BF),
            jax.ShapeDtypeStruct((n_chips, 4, 8, 128), BF),
        ),
        in_specs=[hbm, hbm, hbm, smem],
        out_specs=(hbm, hbm),
        scratch_shapes=[
            pltpu.VMEM(t.shape, BF),
            pltpu.VMEM(w_upper.shape, BF),
            pltpu.VMEM(w_surface.shape, BF),
            pltpu.VMEM((640, 3 * width), BF),
            pltpu.VMEM((320, 2 * width), BF),
            pltpu.VMEM((320, 2 * width), BF),
            pltpu.VMEM((256, 3 * width), BF),
            pltpu.VMEM((128, 2 * width), BF),
            pltpu.VMEM((128, 2 * width), BF),
            pltpu.VMEM((LAT, LAT), BF),
            pltpu.VMEM((640, 256), F32),
            pltpu.VMEM((320, 256), F32),
            dma((t.shape[1] + 2,)),
            pltpu.VMEM((TILES, 3, 8, 128), F32),
            pltpu.VMEM((2, CHANNELS, 8, 128), BF),
            pltpu.VMEM((2, CHANNELS, 8, 128), BF),
            pltpu.VMEM((n_chips, 7, 8, 128), BF),
            dma((2,)),
            dma((2,)),
            dma((2,)),
            dma((2, n_chips)),
            dma((2, n_chips)),
            dma((2, n_chips // SIDE)),
            dma((2, n_chips // SIDE)),
        ],
        compiler_params=pltpu.CompilerParams(
            collective_id=0, has_side_effects=True, vmem_limit_bytes=64 * 10**6
        ),
        name="recover",
    )(t, w_upper, w_surface, bias)
    rows = pl.pallas_call(
        functools.partial(finish, n_chips),
        out_shape=jax.ShapeDtypeStruct((ROWS, 2, n_chips * 24), BF),
        in_specs=[hbm, hbm],
        out_specs=hbm,
        scratch_shapes=[
            pltpu.VMEM((n_chips, 4, 8, 128), BF),
            pltpu.VMEM((n_chips, 4, 8, 128), BF),
            pltpu.VMEM((ROWS, 2, n_chips * 24), BF),
            dma((3,)),
            dma((n_chips // 16,)),
        ],
        compiler_params=pltpu.CompilerParams(vmem_limit_bytes=64 * 10**6),
        name="finish",
    )(got, twin)
    return jnp.transpose(rows, (1, 0, 2))


def solution(mesh):
    n_chips = mesh.shape["win"] // 2
    return jax.shard_map(
        functools.partial(body, n_chips),
        mesh=mesh,
        in_specs=(P("grp", None, None, "win", None), P(), P(), P()),
        out_specs=P("grp", "win", None),
        check_vma=False,
    )
```
